32 devices in a mesh: grp: 4 (over y, x), dev: 8 (over z, core).
Axes of the slice: x: 2, y: 2, z: 4, core: 2. Of those that a mesh axis runs over, the one named last changes fastest.
Arguments:
- examples: float32 [2048, 32768], P(('grp', 'dev'))
- labels: int32 [2048], P(('grp', 'dev')), may hold values from 0 to 1, as said below
Outputs:
- consensus: float32 [32768], replicated
- local_weights: float32 [32, 32768], P(('grp', 'dev'))
- dual_vars: float32 [32, 32768], P(('grp', 'dev'))
The draws below stay inside these ranges and needn't reach their ends.
Inputs may be any that keep to these rules, and one draw needn't show every extreme that they name: `labels`: each example's class, 0 or 1.
All inputs are finite; a program needn't handle non-finite values.
Results may differ from the reference program's by a relative error of at most 0.00012.
Values sent between devices are 32-bit elements; how exact they have to be, the bound alone decides.
No kernel may reach another device: no remote copies, remote signals or barrier semaphores. Data moves between devices by JAX's collectives and lax.ppermute only.
A program may use at most 64 MiB of HBM per device.

```python
import jax
import jax.numpy as jnp
from jax import lax

F = 32768
ROWS = 64
PROX = 3
ROUNDS = 4
TOTAL_ROWS = 2048
N_GRP = 4
N_DEV = 8


def label_keys(key):
    base = jax.random.fold_in(key, 7)
    label_key, noise_key, direction_random_key = jax.random.split(base, 3)
    classes = jax.random.randint(label_key, (TOTAL_ROWS,), 0, 2).astype(jnp.int32)
    return (classes, noise_key, direction_random_key)


def draw_labels(key, part):
    classes, noise_key, direction_random_key = label_keys(key)
    return classes


def draw_examples(key, part):
    classes, noise_key, direction_random_key = label_keys(key)
    direction = jax.random.normal(direction_random_key, (F,), jnp.float32)
    polarity = 2.0 * classes.astype(jnp.float32) - 1.0
    strength = 0.6 / jnp.sqrt(jnp.float32(ROWS))
    noise_part = jax.random.normal(noise_key, (TOTAL_ROWS, F), jnp.float32)
    values = noise_part + strength * polarity[:, None] * direction[None, :]
    values = values / (10.0 * jnp.sqrt(jnp.float32(F)))
    return values.astype(jnp.float32)


def setup_inputs(seed: int = 0) -> dict:
    key_list = jax.random.split(jax.random.key(seed), 3)
    return {
        "examples": draw_examples(jax.random.fold_in(key_list[2], 71), 0),
        "labels": draw_labels(jax.random.fold_in(key_list[2], 71), 0),
    }


step_size = 200.0
penalty = 0.005
thresh = 0.04


def shrink(values):
    return values - jnp.clip(values, -thresh, thresh)


def reference(examples, labels):
    members = N_GRP * N_DEV
    example_blocks = examples.reshape(members, ROWS, F)
    targets = labels.reshape(members, ROWS).astype(jnp.float32)

    def one_round(round_index, carried):
        consensus, weight_vector, dual_vars = carried
        consensus_point = consensus[None, :] - dual_vars
        for prox_index in range(PROX):
            label_margins = jnp.einsum("guz,gz->gu", example_blocks, weight_vector, precision=lax.Precision.HIGHEST)
            primal_residual = jax.nn.sigmoid(label_margins) - targets
            loss_gradient = jnp.einsum("pjl,pj->pl", example_blocks, primal_residual, precision=lax.Precision.HIGHEST)
            weight_vector = (weight_vector - step_size * loss_gradient + step_size * penalty * consensus_point) / (1.0 + step_size * penalty)
        average = jnp.sum(weight_vector + dual_vars, axis=0) / members
        consensus = shrink(average)
        dual_vars = dual_vars + weight_vector - consensus[None, :]
        return consensus, weight_vector, dual_vars

    start = (jnp.zeros((F,), jnp.float32), jnp.zeros((members, F), jnp.float32), jnp.zeros((members, F), jnp.float32))
    consensus, weight_vector, dual_vars = lax.fori_loop(0, ROUNDS, one_round, start)
    return consensus, weight_vector, dual_vars
```

```python
import functools

import jax
import jax.numpy as jnp
from jax import lax
from jax.experimental import pallas as pl
from jax.experimental.pallas import tpu as pltpu
from jax.sharding import PartitionSpec as P

PROX = 3
ROUNDS = 4

step_size = 200.0
penalty = 0.005
thresh = 0.04

DENOM = 1.0 + step_size * penalty
PULL = step_size * penalty / DENOM
KEEP = 1.0 / DENOM
GRAD = step_size / DENOM
KEEP_ALL = KEEP**PROX
PULL_ALL = PULL * sum(KEEP**s for s in range(PROX))
GRAD_AT = [GRAD * KEEP ** (PROX - 1 - s) for s in range(PROX)]

LANES = 128
SUB = 8
STEP = LANES * SUB
AXES = ("grp", "dev")
F32 = jnp.float32
SCRATCH_BYTES = 8 << 20


def vmem(x):
    return pltpu.with_memory_space_constraint(x, pltpu.VMEM)


def shrink(values):
    return values - jnp.clip(values, -thresh, thresh)


def half_of():
    group = lax.axis_index("grp")
    bits = lax.axis_index("dev")
    for shift in range(max(1, (lax.axis_size("grp") - 1).bit_length())):
        bits = bits + (group >> shift)
    return bits & 1


def column(row):
    rows = row.shape[1]
    eye = lax.broadcasted_iota(jnp.int32, (rows, rows), 0) == lax.broadcasted_iota(jnp.int32, (rows, rows), 1)
    picked = jnp.where(eye, jnp.broadcast_to(row, (rows, rows)), 0.0)
    return jnp.broadcast_to(jnp.sum(picked, axis=1, keepdims=True), (rows, LANES))


def lanes_sum(values):
    return jnp.broadcast_to(jnp.sum(values, axis=1, keepdims=True), values.shape)


def gram_times(gram, residual):
    rows = gram.shape[0]
    row = jnp.sum(gram * residual, axis=0, keepdims=True)
    eye = lax.broadcasted_iota(jnp.int32, gram.shape, 0) == lax.broadcasted_iota(jnp.int32, gram.shape, 1)
    return lanes_sum(jnp.where(eye, jnp.broadcast_to(row, gram.shape), 0.0))


def blocks(x_ref, step):
    for j in range(SUB):
        yield j, x_ref[:, pl.ds(pl.multiple_of(step * STEP + j * LANES, LANES), LANES)]


def times_vector(x_ref, vec_ref, steps):
    def body(step, acc):
        vec = vec_ref[pl.ds(pl.multiple_of(step * SUB, SUB), SUB), :]
        for j, x in blocks(x_ref, step):
            acc = acc + x * vec[j : j + 1, :]
        return acc

    zero = jnp.zeros((x_ref.shape[0], LANES), F32)
    return lanes_sum(lax.fori_loop(0, steps, body, zero, unroll=2))


def transposed_times(x_ref, coef, out_ref, first, steps):
    def body(i, carry):
        rows = [jnp.sum(x * coef, axis=0, keepdims=True) for _, x in blocks(x_ref, first + i)]
        out_ref[pl.ds(pl.multiple_of(i * SUB, SUB), SUB), :] = jnp.concatenate(rows, axis=0)
        return carry

    lax.fori_loop(0, steps, body, 0, unroll=2)


def forth_and_back(x_ref, coef, first, steps, acc):
    def body(i, acc):
        for _, x in blocks(x_ref, first + i):
            acc = acc + x * jnp.sum(x * coef, axis=0, keepdims=True)
        return acc

    return lax.fori_loop(0, steps, body, acc, unroll=2)


def halves_out(x_ref, coef, keep_ref, send_ref, half, steps):
    transposed_times(x_ref, coef, send_ref, (1 - half) * (steps // 2), steps // 2)
    transposed_times(x_ref, coef, keep_ref, half * (steps // 2), steps // 2)


def first_kernel(chunks, steps, x_hbm, label_ref, x_ref, keep_ref, send_ref, coef_ref, target_ref, sems):
    half = half_of()
    rows, width = x_ref.shape
    cols = width // chunks

    def fetch(i):
        span = pl.ds(i * cols, cols)
        return pltpu.make_async_copy(x_hbm.at[:, span], x_ref.at[:, span], sems.at[i])

    for i in range(chunks):
        fetch(i).start()
    target = column(label_ref[...].astype(F32))
    target_ref[...] = target
    residual = 0.5 - target
    coef = GRAD_AT[0] * residual
    acc = jnp.zeros((rows, LANES), F32)
    per = steps // chunks
    for i in range(chunks):
        fetch(i).wait()
        acc = forth_and_back(x_ref, residual, i * per, per, acc)
    margin = -GRAD * lanes_sum(acc)
    for s in range(1, PROX):
        residual = jax.nn.sigmoid(margin) - target
        coef = coef + GRAD_AT[s] * residual
        if s + 1 < PROX:
            acc = forth_and_back(x_ref, residual, 0, steps, jnp.zeros((rows, LANES), F32))
            margin = KEEP * margin - GRAD * lanes_sum(acc)
    coef_ref[...] = coef
    halves_out(x_ref, coef, keep_ref, send_ref, half, steps)


def gram_kernel(steps, x_ref, coef_ref, gram_ref, margin_ref):
    rows = x_ref.shape[0]

    def body(i, acc):
        x = x_ref[:, pl.ds(pl.multiple_of(i * STEP, STEP), STEP)]
        high = x.astype(jnp.bfloat16)
        low = (x - high.astype(F32)).astype(jnp.bfloat16)
        both = jnp.concatenate([high, low], axis=0)
        return acc + lax.dot_general(both, both, (((1,), (1,)), ((), ())), preferred_element_type=F32)

    prod = lax.fori_loop(0, steps, body, jnp.zeros((2 * rows, 2 * rows), F32), unroll=2)
    prod = prod[:rows] + prod[rows:]
    gram = prod + pltpu.roll(prod, rows, 1)
    gram_ref[...] = gram
    margin_ref[...] = -gram_times(gram, coef_ref[...])


def round_kernel(
    steps,
    members,
    x_ref,
    own_ref,
    other_ref,
    z_in,
    u_in,
    w_in,
    gram_ref,
    mw_in,
    mu_in,
    target_ref,
    keep_ref,
    send_ref,
    z_ref,
    u_ref,
    w_ref,
    mw_ref,
    mu_ref,
):
    half = half_of()
    count = own_ref.shape[0]
    for ref, at in ((own_ref, half), (other_ref, 1 - half)):
        span = pl.ds(pl.multiple_of(at * count, count), count)
        u_old = u_in[span, :]
        w_new = KEEP_ALL * w_in[span, :] + PULL_ALL * (z_in[span, :] - u_old) - ref[...] * (1.0 / members)
        average = w_new + u_old
        z_new = shrink(average)
        z_ref[span, :] = z_new
        u_ref[span, :] = average - z_new
        w_ref[span, :] = w_new
    xz = times_vector(x_ref, z_ref, steps)
    gram = gram_ref[...]
    target = target_ref[...]
    margin = mw_in[...]
    mu = mu_in[...] + margin - xz
    mu_ref[...] = mu
    pull = PULL * (xz - mu)
    coef = None
    for s in range(PROX):
        residual = jax.nn.sigmoid(margin) - target
        part = GRAD_AT[s] * residual
        coef = part if coef is None else coef + part
        margin = KEEP * margin + pull - GRAD * gram_times(gram, residual)
    mw_ref[...] = margin
    halves_out(x_ref, coef, keep_ref, send_ref, half, steps)


def last_kernel(members, own_ref, other_ref, z_in, u_in, w_in, sum_ref, z_ref, dual_ref):
    half = half_of()
    count = own_ref.shape[0]
    for ref, at in ((own_ref, half), (other_ref, 1 - half)):
        span = pl.ds(pl.multiple_of(at * count, count), count)
        u_old = u_in[span, :]
        w_new = KEEP_ALL * w_in[span, :] + PULL_ALL * (z_in[span, :] - u_old) - ref[...] * (1.0 / members)
        z_new = shrink(w_new + u_old)
        z_ref[span, :] = z_new
        dual_ref[span, :] = sum_ref[span, :] - z_new


def local_kernel(keep_ref, send_ref, z_ref, u_in, w_in, u_ref, w_ref, both_ref):
    half = half_of()
    count = keep_ref.shape[0]
    for ref, at in ((keep_ref, half), (send_ref, 1 - half)):
        span = pl.ds(pl.multiple_of(at * count, count), count)
        z = z_ref[span, :]
        w_old = w_in[span, :]
        u = u_in[span, :] + w_old - z
        w = KEEP_ALL * w_old + PULL_ALL * (z - u) - ref[...]
        u_ref[span, :] = u
        w_ref[span, :] = w
        both_ref[span, :] = u + w


def exchange(values, mask, members):
    return lax.ppermute(values, AXES, [(i, i ^ mask) for i in range(members)])


def stages(n_grp, n_dev):
    found = []
    bits = [n_dev << b for b in range(n_grp.bit_length() - 1)]
    for i in range(0, len(bits), 2):
        pair = bits[i : i + 2]
        found.append([b | 1 for b in pair] + ([sum(pair)] if len(pair) > 1 else []))
    bits = [1 << b for b in range(1, n_dev.bit_length() - 1)]
    for i in range(0, len(bits), 2):
        pair = bits[i : i + 2]
        found.append(pair[::-1] + ([sum(pair)] if len(pair) > 1 else []))
    return found


def sum_halves(keep, send, n_grp, n_dev):
    members = n_grp * n_dev
    total = keep + exchange(send, 1, members)
    for masks in stages(n_grp, n_dev):
        got = [exchange(total, mask, members) for mask in masks]
        if len(got) == 3:
            total = (total + got[0]) + (got[1] + got[2])
        else:
            total = total + got[0]
    return total, exchange(total, 1, members)


def per_device(examples, labels):
    n_grp, n_dev = lax.axis_size("grp"), lax.axis_size("dev")
    members = n_grp * n_dev
    rows, width = examples.shape
    if n_grp & (n_grp - 1) or n_dev & (n_dev - 1) or n_dev < 2:
        raise ValueError("mesh axes")
    steps = width // STEP
    lines = width // LANES
    chunks = 8
    small = pltpu.VMEM((rows, LANES), F32)
    half = pltpu.VMEM((lines // 2, LANES), F32)
    full = pltpu.VMEM((lines, LANES), F32)
    here = pl.BlockSpec(memory_space=pltpu.VMEM)

    def call(body, outs, n_in, **kw):
        params = pltpu.CompilerParams(vmem_limit_bytes=SCRATCH_BYTES)
        return pl.pallas_call(body, compiler_params=params, out_shape=outs, in_specs=kw.pop("in_specs", [here] * n_in), out_specs=[here] * len(outs), **kw)

    x, keep, send, coef, target = call(
        functools.partial(first_kernel, chunks, steps),
        [pltpu.VMEM((rows, width), F32), half, half, small, small],
        2,
        in_specs=[pl.BlockSpec(memory_space=pltpu.HBM), here],
        scratch_shapes=[pltpu.SemaphoreType.DMA((chunks,))],
        name="first",
    )(pltpu.with_memory_space_constraint(examples, pltpu.HBM), labels.reshape(1, rows))
    gram, mw = call(functools.partial(gram_kernel, steps), [small, small], 2, name="gram")(vmem(x), coef)
    mu = jnp.zeros((rows, LANES), F32)
    z = jnp.zeros((lines, LANES), F32)
    u = z
    w = z

    local_u = local_w = z
    for turn in range(ROUNDS):
        local_u, local_w, both = call(local_kernel, [full, full, full], 5, name="local")(keep, send, z, local_u, local_w)
        own, other = sum_halves(keep, send, n_grp, n_dev)
        if turn + 1 == ROUNDS:
            break
        keep, send, z, u, w, mw, mu = call(
            functools.partial(round_kernel, steps, members),
            [half, half, full, full, full, small, small],
            10,
            name="round",
        )(vmem(x), own, other, z, u, w, gram, mw, mu, target)
    out = jax.ShapeDtypeStruct((lines, LANES), F32)
    z, dual = call(functools.partial(last_kernel, members), [out, out], 6, name="last")(
        own, other, z, u, w, both
    )
    return z.reshape(width), local_w.reshape(1, width), dual.reshape(1, width)


def solution(mesh):
    placed = (P(AXES, None), P(AXES))
    return jax.shard_map(
        per_device,
        mesh=mesh,
        in_specs=placed,
        out_specs=(P(), P(AXES, None), P(AXES, None)),
        check_vma=False,
    )
```

```python
import functools

import jax
import jax.numpy as jnp
from jax import lax
from jax.experimental import pallas as pl
from jax.experimental.pallas import tpu as pltpu
from jax.sharding import PartitionSpec as P


PROX = 3
ROUNDS = 4

step_size = 200.0
penalty = 0.005
thresh = 0.04

DENOM = 1.0 + step_size * penalty
PULL = step_size * penalty / DENOM
KEEP = 1.0 / DENOM
GRAD = step_size / DENOM
KEEP_ALL = KEEP**PROX
PULL_ALL = PULL * sum(KEEP**s for s in range(PROX))
GRAD_AT = [GRAD * KEEP ** (PROX - 1 - s) for s in range(PROX)]

LANES = 128
SUB = 8
AXES = ("grp", "dev")
F32 = jnp.float32
SCRATCH_BYTES = 8 << 20


def vmem(x):
    return pltpu.with_memory_space_constraint(x, pltpu.VMEM)


def shrink(values):
    return values - jnp.clip(values, -thresh, thresh)


def half_of():
    group = lax.axis_index("grp")
    bits = lax.axis_index("dev")
    for shift in range(max(1, (lax.axis_size("grp") - 1).bit_length())):
        bits = bits + (group >> shift)
    return bits & 1


def eye_mask(shape):
    return lax.broadcasted_iota(jnp.int32, shape, 0) == lax.broadcasted_iota(jnp.int32, shape, 1)


def column(row):
    rows = row.shape[1]
    picked = jnp.where(eye_mask((rows, rows)), jnp.broadcast_to(row, (rows, rows)), 0.0)
    return jnp.broadcast_to(jnp.sum(picked, axis=1, keepdims=True), (rows, LANES))


def lanes_sum(values):
    return jnp.broadcast_to(jnp.sum(values, axis=1, keepdims=True), values.shape)


def gram_times(gram, residual):
    row = jnp.sum(gram * residual, axis=0, keepdims=True)
    return lanes_sum(jnp.where(eye_mask(gram.shape), jnp.broadcast_to(row, gram.shape), 0.0))


def strip(i):
    return pl.ds(pl.multiple_of(i * SUB, SUB), SUB)


def times_vector(refs, vec_ref):
    def body(i, accs):
        vec = vec_ref[strip(i), :]
        accs = list(accs)
        for j in range(SUB):
            for n, ref in enumerate(refs):
                accs[n] = accs[n] + ref[i * SUB + j] * vec[j : j + 1, :]
        return tuple(accs)

    zero = jnp.zeros(refs[0].shape[1:], F32)
    return lax.fori_loop(0, refs[0].shape[0] // SUB, body, (zero,) * len(refs))


def transposed_times(pairs, out_ref):
    def body(i, carry):
        rows = []
        for j in range(SUB):
            terms = [ref[i * SUB + j] * coef for ref, coef in pairs]
            rows.append(jnp.sum(functools.reduce(jnp.add, terms), axis=0, keepdims=True))
        out_ref[strip(i), :] = jnp.concatenate(rows, axis=0)
        return carry

    lax.fori_loop(0, out_ref.shape[0] // SUB, body, 0, unroll=2)


def forth_and_back(ref, first, count, coef, acc):
    def body(i, acc):
        for j in range(SUB):
            x = ref[first + i * SUB + j]
            acc = acc + x * jnp.sum(x * coef, axis=0, keepdims=True)
        return acc

    return lax.fori_loop(0, count // SUB, body, acc, unroll=2)


def first_kernel(chunks, x_hbm, label_ref, keep_x, send_x, keep_ref, send_ref, coef_ref, target_ref, sems):
    half = half_of()
    count, rows, _ = keep_x.shape
    tiles = rows // SUB
    per = count // chunks

    def fetch(n, i, t):
        ref, at = ((keep_x, half), (send_x, 1 - half))[n]
        return pltpu.make_async_copy(
            x_hbm.at[t, pl.ds(at * count + i * per, per)],
            ref.at[pl.ds(i * per, per), pl.ds(t * SUB, SUB)],
            sems.at[n, i, t],
        )

    places = [(n, i) for n in range(2) for i in range(chunks)]
    for n, i in places:
        for t in range(tiles):
            fetch(n, i, t).start()
    target = column(label_ref[...].astype(F32))
    target_ref[...] = target
    residual = 0.5 - target
    coef = GRAD_AT[0] * residual
    zero = jnp.zeros((rows, LANES), F32)
    acc = zero
    for n, i in places:
        for t in range(tiles):
            fetch(n, i, t).wait()
        acc = forth_and_back((keep_x, send_x)[n], i * per, per, residual, acc)
    margin = -GRAD * lanes_sum(acc)
    for s in range(1, PROX):
        residual = jax.nn.sigmoid(margin) - target
        coef = coef + GRAD_AT[s] * residual
        if s + 1 < PROX:
            acc = forth_and_back(keep_x, 0, count, residual, zero)
            acc = forth_and_back(send_x, 0, count, residual, acc)
            margin = KEEP * margin - GRAD * lanes_sum(acc)
    coef_ref[...] = coef
    transposed_times([(send_x, coef)], send_ref)
    transposed_times([(keep_x, coef)], keep_ref)


def gram_kernel(keep_x, send_x, coef_ref, target_ref, pack_ref):
    count, rows, _ = keep_x.shape

    def body(i, acc):
        for ref in (keep_x, send_x):
            for j in range(0, SUB, 2):
                x = jnp.concatenate([ref[i * SUB + j], ref[i * SUB + j + 1]], axis=1)
                high = x.astype(jnp.bfloat16)
                low = (x - high.astype(F32)).astype(jnp.bfloat16)
                both = jnp.concatenate([high, low], axis=0)
                acc = acc + lax.dot_general(both, both, (((1,), (1,)), ((), ())), preferred_element_type=F32)
        return acc

    prod = lax.fori_loop(0, count // SUB, body, jnp.zeros((2 * rows, 2 * rows), F32))
    prod = prod[:rows] + prod[rows:]
    gram = prod + pltpu.roll(prod, rows, 1)
    pack_ref[:rows] = gram
    pack_ref[rows : 2 * rows] = -gram_times(gram, coef_ref[...])
    pack_ref[2 * rows :] = target_ref[...]


def point_kernel(members, keep_x, other_x, sum_ref, z_in, u_in, w_in, z_ref, u_ref, w_ref, part_ref):
    rows = keep_x.shape[1]
    u_old = u_in[...]
    w_new = KEEP_ALL * w_in[...] + PULL_ALL * (z_in[...] - u_old) - sum_ref[...] * (1.0 / members)
    average = w_new + u_old
    z_new = shrink(average)
    z_ref[...] = z_new
    u_ref[...] = average - z_new
    w_ref[...] = w_new
    mine, others = times_vector([keep_x, other_x], z_ref)
    part_ref[:rows] = mine
    part_ref[rows:] = others


def prox_kernel(fresh, keep_x, other_x, part_ref, got_ref, own_pack, other_pack, state_in, out_ref, coef_ref, state_ref=None):
    rows = keep_x.shape[1]
    part = part_ref[...]
    got = got_ref[...]
    whole = [part[:rows] + got[rows:], part[rows:] + got[:rows]]
    coefs = []
    for n, pack in enumerate((own_pack, other_pack)):
        at = pl.ds(n * rows, rows)
        mu_at = pl.ds((2 + n) * rows, rows)
        xz = lanes_sum(whole[n])
        gram = pack[:rows]
        target = pack[2 * rows :]
        if fresh:
            margin = pack[rows : 2 * rows]
            mu = margin - xz
        else:
            margin = state_in[at]
            mu = state_in[mu_at] + margin - xz
        pull = PULL * (xz - mu)
        coef = None
        for s in range(PROX):
            residual = jax.nn.sigmoid(margin) - target
            term = GRAD_AT[s] * residual
            coef = term if coef is None else coef + term
            margin = KEEP * margin + pull - GRAD * gram_times(gram, residual)
        if state_ref is not None:
            state_ref[at] = margin
            state_ref[mu_at] = mu
        coefs.append(coef)
    coef_ref[...] = coefs[0]
    transposed_times([(keep_x, coefs[0]), (other_x, coefs[1])], out_ref)


def affine_kernel(u_mean, w_mean, *refs):
    z_refs, out_ref = refs[:-1], refs[-1]
    count = u_mean.shape[0]
    w = u = z = jnp.zeros((count, LANES), F32)
    for z_ref in z_refs:
        w = KEEP_ALL * w + PULL_ALL * (z - u)
        z = z_ref[...]
        u = u + w - z
    w = KEEP_ALL * w + PULL_ALL * (z - u)
    out_ref[:count] = w
    out_ref[count : 2 * count] = u + w
    mean = u_mean[...]
    out_ref[2 * count :] = KEEP_ALL * w_mean[...] + PULL_ALL * (z - mean) + mean


def local_kernel(keep_x, send_x, own_ref, other_ref, *refs):
    coef_refs, (w_ref, both_ref) = refs[:-2], refs[-2:]
    half = half_of()
    count, rows, _ = keep_x.shape
    cw = cu = jnp.zeros((rows, LANES), F32)
    for coef_ref in coef_refs:
        cw = KEEP_ALL * cw - PULL_ALL * cu + coef_ref[...]
        cs = cu + cw
        cu = cs
    for x_ref, z_ref, at in ((keep_x, own_ref, half), (send_x, other_ref, 1 - half)):

        def body(i, carry, x_ref=x_ref, z_ref=z_ref, at=at):
            rows_w, rows_s = [], []
            for j in range(SUB):
                x = x_ref[i * SUB + j]
                rows_w.append(jnp.sum(x * cw, axis=0, keepdims=True))
                rows_s.append(jnp.sum(x * cs, axis=0, keepdims=True))
            to = strip(at * (count // SUB) + i)
            w_ref[to, :] = z_ref[strip(i), :] - jnp.concatenate(rows_w, axis=0)
            both_ref[to, :] = z_ref[strip(count // SUB + i), :] - jnp.concatenate(rows_s, axis=0)
            return carry

        lax.fori_loop(0, count // SUB, body, 0)


def last_kernel(members, own_ref, other_ref, own_base, other_base, both_ref, z_ref, dual_ref):
    half = half_of()
    count = own_ref.shape[0]
    for ref, base, at in ((own_ref, own_base, half), (other_ref, other_base, 1 - half)):
        span = pl.ds(pl.multiple_of(at * count, count), count)
        z_new = shrink(base[2 * count :] - ref[...] * (1.0 / members))
        z_ref[span, :] = z_new
        dual_ref[span, :] = both_ref[span, :] - z_new


def exchange(values, mask):
    members = lax.axis_size("grp") * lax.axis_size("dev")
    return lax.ppermute(values, AXES, [(i, i ^ mask) for i in range(members)])


def stages(n_grp, n_dev):
    found = []
    bits = [n_dev << b for b in range(n_grp.bit_length() - 1)]
    for i in range(0, len(bits), 2):
        pair = bits[i : i + 2]
        found.append([b | 1 for b in pair] + ([sum(pair)] if len(pair) > 1 else []))
    bits = [1 << b for b in range(1, n_dev.bit_length() - 1)]
    for i in range(0, len(bits), 2):
        pair = bits[i : i + 2]
        found.append(pair[::-1] + ([sum(pair)] if len(pair) > 1 else []))
    return found


def sum_chips(total, n_grp, n_dev):
    plan = stages(n_grp, n_dev)
    for masks in plan:
        got = [exchange(total, mask) for mask in masks]
        if len(got) == 3:
            total = (total + got[0]) + (got[1] + got[2])
        else:
            total = total + got[0]
    return total


def call(body, outs, n_in, **kw):
    here = pl.BlockSpec(memory_space=pltpu.VMEM)
    params = pltpu.CompilerParams(vmem_limit_bytes=SCRATCH_BYTES)
    specs = kw.pop("in_specs", [here] * n_in)
    return pl.pallas_call(body, compiler_params=params, out_shape=outs, in_specs=specs, out_specs=[here] * len(outs), **kw)


def per_device(examples, labels):
    n_grp, n_dev = lax.axis_size("grp"), lax.axis_size("dev")
    members = n_grp * n_dev
    rows, width = examples.shape
    if n_grp & (n_grp - 1) or n_dev & (n_dev - 1) or n_dev < 2:
        raise ValueError("mesh axes")
    blocks = width // LANES
    count = blocks // 2
    tiles = rows // SUB
    chunks = 4
    small = pltpu.VMEM((rows, LANES), F32)
    double = pltpu.VMEM((2 * rows, LANES), F32)
    half = pltpu.VMEM((count, LANES), F32)
    x_half = pltpu.VMEM((count, rows, LANES), F32)
    out = jax.ShapeDtypeStruct((blocks, LANES), F32)

    tiled = examples.reshape(tiles, SUB, blocks, LANES).transpose(0, 2, 1, 3)
    keep_x, send_x, keep, send, coef, target = call(
        functools.partial(first_kernel, chunks),
        [x_half, x_half, half, half, small, small],
        2,
        in_specs=[pl.BlockSpec(memory_space=pltpu.HBM), pl.BlockSpec(memory_space=pltpu.VMEM)],
        scratch_shapes=[pltpu.SemaphoreType.DMA((2, chunks, tiles))],
        name="first",
    )(pltpu.with_memory_space_constraint(tiled, pltpu.HBM), labels.reshape(1, rows))
    keep_x = vmem(keep_x)
    send_x = vmem(send_x)
    got = exchange(send, 1)
    got, moved = lax.optimization_barrier((got, send_x))
    other_x = vmem(exchange(moved, 1))
    total = keep + got
    (own_pack,) = call(gram_kernel, [pltpu.VMEM((3 * rows, LANES), F32)], 4, name="gram")(keep_x, send_x, coef, target)
    other_pack = exchange(own_pack, 1)
    z = u = w = jnp.zeros((count, LANES), F32)
    state = [jnp.zeros((4 * rows, LANES), F32)]
    coefs = [coef]
    points = []
    for turn in range(1, ROUNDS):
        total = sum_chips(total, n_grp, n_dev)
        z, u, w, part = call(functools.partial(point_kernel, members), [half, half, half, double], 6, name="point")(
            keep_x, other_x, total, z, u, w
        )
        points.append(z)
        got = exchange(part, 1)
        kept = [pltpu.VMEM((4 * rows, LANES), F32)] if turn + 1 < ROUNDS else []
        total, coef, *state = call(functools.partial(prox_kernel, turn == 1), [half, small, *kept], 7, name="prox")(
            keep_x, other_x, part, got, own_pack, other_pack, *state
        )
        coefs.append(coef)
    (own_base,) = call(affine_kernel, [pltpu.VMEM((3 * count, LANES), F32)], 2 + len(points), name="affine")(u, w, *points)
    other_base = exchange(own_base, 1)
    local_w, both = call(local_kernel, [out, pltpu.VMEM((blocks, LANES), F32)], 4 + len(coefs), name="local")(
        keep_x, send_x, own_base, other_base, *coefs
    )
    total = sum_chips(total, n_grp, n_dev)
    z, dual = call(functools.partial(last_kernel, members), [out, out], 5, name="last")(
        total, exchange(total, 1), own_base, other_base, both
    )
    return z.reshape(width), local_w.reshape(1, width), dual.reshape(1, width)


def solution(mesh):
    placed = (P(AXES, None), P(AXES))
    return jax.shard_map(
        per_device,
        mesh=mesh,
        in_specs=placed,
        out_specs=(P(), P(AXES, None), P(AXES, None)),
        check_vma=False,
    )
```
